256 devices in a mesh: groups: 2 (over y), seq: 16 (over z), tensor: 4 (over x), cfg: 2 (over core).
Axes of the slice: x: 4, y: 2, z: 16, core: 2. Of those that a mesh axis runs over, the one named last changes fastest.
The devices are a block of a 4x16x16 slice.
Arguments:
- latent: bfloat16 [8192, 3072], P(('groups', 'seq')), parts along dimension 0, may hold values from -6 to 6
- positions: int32 [3, 8192], P(None, ('groups', 'seq')), parts along dimension 1, may hold values from 0 to 79, as said below
- text_kv: bfloat16 [2, 2, 512, 3072], P('cfg', None, ('groups', 'seq'), 'tensor'), parts along dimension 2, may hold values from -6 to 6
- text_len: int32 [4], P(('groups', 'cfg')), parts along dimension 0, may hold values from 1 to 256
- modulation: float32 [3, 4, 3072], P(None, 'groups'), parts along dimension 1, may hold values from -3 to 3
- w_qkv: bfloat16 [3, 3072, 3072], P(None, 'cfg', 'tensor'), may hold values from -0.109375 to 0.109375
- norm_gains: float32 [2, 128], replicated, may hold values from 0.5 to 2.5
- w_out: bfloat16 [3072, 3072], P('tensor', 'cfg'), may hold values from -0.109375 to 0.109375
- guidance: float32 [2], P('groups'), parts along dimension 0, may hold values from 3 to 8
Outputs:
- guided: bfloat16 [8192, 3072], P(('groups', 'seq', 'tensor'), 'cfg'), parts along dimension 0
The draws below stay inside these ranges and needn't reach their ends.
There are 2 independent parts, one for each index of `groups`. The reference program is written for one: setup_inputs(seed, part) draws one part's arguments, and reference() takes and returns one part's arrays. A program takes and returns all parts, laid end to end along the dimension named above; an argument that names none is the same for every part. Nothing has to cross between parts.
Inputs may be any that keep to these rules, and one draw needn't show every extreme that they name: `positions`: frame indices are below 33, height indices below 45, width indices below 80. `text_len`: text rows at or beyond the count are ignored.
All inputs are finite; a program needn't handle non-finite values.
Results may differ from the reference program's by a relative error of at most 0.018.
Values may be sent and summed in bfloat16 or wider, within the bound.
A program may use at most 128 MiB of HBM per device.

```python
import math
import jax
import jax.numpy as jnp
from jax import lax

D = 3072
HEADS = 24
HEAD_DIM = 128
TOKENS = 4096
TEXT = 256


def draw_positions(key, part):
    keys = jax.random.split(jax.random.fold_in(key, 11), 3)
    frame = jax.random.randint(keys[0], (TOKENS,), 0, 33)
    height = jax.random.randint(keys[1], (TOKENS,), 0, 45)
    across = jax.random.randint(keys[2], (TOKENS,), 0, 80)
    return jnp.stack([frame, height, across]).astype(jnp.int32)


def level_of(stream_key, extent, cuts, smallest, largest):
    level, own = 1.0, jax.random.fold_in(stream_key, 6)
    for dim, shards_of in cuts:
        heights = jnp.exp(jax.random.uniform(jax.random.fold_in(own, dim), (shards_of,), jnp.float32, smallest / len(cuts), largest / len(cuts)))
        level = level * jnp.repeat(heights, extent[dim] // shards_of).reshape([-1 if axis == dim else 1 for axis in range(len(extent))])
    return level


def normal_values(stream_key, extent, scale, bound, cuts=(), kind=jnp.bfloat16):
    entries = jax.random.normal(stream_key, extent, jnp.float32) * scale
    if len(cuts) > 0:
        entries = level_of(stream_key, extent, cuts, -0.22, 0.18) * entries
    return jnp.clip(entries, min=-bound, max=bound).astype(kind)


def setup_inputs(seed: int = 0, part: int = 0) -> dict:
    splits = jax.random.split(jax.random.key(seed), 10)
    own_keys = jax.random.split(jax.random.fold_in(splits[9], part), 10)
    return {
        "latent": normal_values(own_keys[0], (TOKENS, D), 1.0, 6.0, ((0, 16),)),
        "positions": draw_positions(jax.random.fold_in(jax.random.fold_in(splits[9], part), 71), part),
        "text_kv": normal_values(own_keys[2], (2, 2, TEXT, D), 1.0, 6.0, ((0, 2), (2, 16), (3, 4))),
        "text_len": jax.random.randint(own_keys[3], (2,), 1, TEXT + 1).astype(jnp.int32),
        "modulation": normal_values(own_keys[4], (3, 2, D), 0.5, 3.0, (), jnp.float32),
        "w_qkv": normal_values(splits[5], (3, D, D), D ** -0.5, 0.109375, ((1, 2), (2, 4))),
        "norm_gains": jnp.clip(jnp.exp(jax.random.uniform(splits[6], (2, HEAD_DIM), jnp.float32, math.log(0.5), math.log(2.5))), 0.5, 2.5),
        "w_out": normal_values(splits[7], (D, D), D ** -0.5, 0.109375, ((0, 4), (1, 2))),
        "guidance": jnp.clip(jax.random.uniform(own_keys[8], (1,), jnp.float32, 3.0, 8.0), 3.0, 8.0),
    }


def head_norm(heads_in, gain):
    return heads_in * lax.rsqrt(lax.optimization_barrier(jnp.mean(heads_in * heads_in, axis=-1, keepdims=True)) + 1e-06) * gain

def rotary(heads_in, positions):
    head_size = heads_in.shape[-1]
    blocks = (head_size // 8, 7 * head_size // 16, 7 * head_size // 16)
    pieces = []
    offset = 0
    for axis_id in range(3):
        width = blocks[axis_id]
        half = width // 2
        freq = 256.0 ** (-jnp.arange(half, dtype=jnp.float32) / half)
        angle = positions[axis_id].astype(jnp.float32)[:, None] * freq[None, :]
        cosine = jnp.cos(angle)[:, None, :]
        sine = jnp.sin(angle)[:, None, :]
        first = heads_in[..., offset:offset + half]
        second = heads_in[..., offset + half:offset + width]
        pieces.append(first * cosine - second * sine)
        pieces.append(second * cosine + first * sine)
        offset = offset + width
    return jnp.concatenate(pieces, axis=-1)

def reference(latent, positions, text_kv, text_len, modulation, w_qkv, norm_gains, w_out, guidance):
    rows = latent.shape[0]
    xfloat = latent.astype(jnp.float32)
    center = xfloat - lax.optimization_barrier(jnp.mean(xfloat, axis=-1, keepdims=True))
    normed = center * lax.rsqrt(lax.optimization_barrier(jnp.mean(center * center, axis=-1, keepdims=True)) + 1e-06)
    scale = HEAD_DIM ** (-0.5)
    outputs = []
    for branch in range(2):
        modulated = (normed * (1.0 + modulation[1, branch]) + modulation[0, branch]).astype(jnp.bfloat16)
        projected = [jnp.dot(modulated, w_qkv[j], preferred_element_type=jnp.float32) for j in range(3)]
        queries = rotary(head_norm(projected[0].reshape(rows, HEADS, HEAD_DIM), norm_gains[0]), positions).astype(jnp.bfloat16)
        keys = rotary(head_norm(projected[1].reshape(rows, HEADS, HEAD_DIM), norm_gains[1]), positions).astype(jnp.bfloat16)
        value_rows = projected[2].astype(jnp.bfloat16).reshape(rows, HEADS, HEAD_DIM)
        prompt_keys = head_norm(text_kv[branch, 0].astype(jnp.float32).reshape(TEXT, HEADS, HEAD_DIM), norm_gains[1]).astype(jnp.bfloat16)
        all_keys = jnp.concatenate([keys, prompt_keys], axis=0)
        all_values = jnp.concatenate([value_rows, text_kv[branch, 1].reshape(TEXT, HEADS, HEAD_DIM)], axis=0)
        valid = jnp.concatenate([jnp.ones((rows,), bool), jnp.arange(TEXT, dtype=jnp.int32) < text_len[branch]])

        def one_head(operands):
            query_head, key_head, value_head = operands
            scores = jnp.dot(query_head, key_head.T, preferred_element_type=jnp.float32) * scale
            expo = jnp.where(valid[None, :], jnp.exp(scores), 0.0)
            total = lax.optimization_barrier(jnp.sum(expo, axis=-1, keepdims=True))
            mixed = jnp.dot(expo.astype(jnp.bfloat16), value_head, preferred_element_type=jnp.float32)
            return mixed / total
        attended = lax.map(one_head, (queries.transpose(1, 0, 2), all_keys.transpose(1, 0, 2), all_values.transpose(1, 0, 2)))
        attended = attended.transpose(1, 0, 2).reshape(rows, HEADS * HEAD_DIM).astype(jnp.bfloat16)
        branch_out = (modulation[2, branch] * jnp.dot(attended, w_out, preferred_element_type=jnp.float32)).astype(jnp.bfloat16)
        outputs.append(lax.optimization_barrier(branch_out).astype(jnp.float32))
    return (outputs[1] + guidance[0] * (outputs[0] - outputs[1])).astype(jnp.bfloat16)
```

```python
import functools

import jax
import jax.numpy as jnp
import numpy as np
from jax import lax
from jax.experimental import pallas as pl
from jax.experimental.pallas import tpu as pltpu
from jax.sharding import PartitionSpec as P

HEAD_DIM = 128
MESH = pl.DeviceIdType.MESH
F32 = jnp.float32
BF16 = jnp.bfloat16
STARTS = (0, 40, 96)
LIMITS = (33, 45, 80)
TABLE_ROWS = 256
BLOCKS = (16, 56, 56)


def rotary_table():
    table = np.zeros((TABLE_ROWS, 2 * HEAD_DIM), np.float32)
    offset = 0
    for start, limit, width in zip(STARTS, LIMITS, BLOCKS):
        half = width // 2
        freq = (256.0 ** (-np.arange(half, dtype=np.float64) / half)).astype(np.float32)
        angle = np.arange(limit, dtype=np.float32)[:, None] * freq[None, :]
        cosine, sine = np.cos(angle.astype(np.float64)), np.sin(angle.astype(np.float64))
        rows = slice(start, start + limit)
        table[rows, offset : offset + half] = cosine
        table[rows, offset + half : offset + width] = cosine
        table[rows, HEAD_DIM + offset : HEAD_DIM + offset + half] = -sine
        table[rows, HEAD_DIM + offset + half : HEAD_DIM + offset + width] = sine
        offset += width
    high = jnp.asarray(table).astype(BF16)
    low = (jnp.asarray(table) - high.astype(F32)).astype(BF16)
    return jnp.concatenate([high, low], axis=0)


def partner_lanes(x):
    lane = lax.broadcasted_iota(jnp.int32, x.shape, 1)
    small, large = BLOCKS[0] // 2, BLOCKS[1] // 2
    wide_first = ((lane >= 16) & (lane < 44)) | ((lane >= 72) & (lane < 100))
    wide = jnp.where(
        wide_first, pltpu.roll(x, HEAD_DIM - large, 1), pltpu.roll(x, large, 1)
    )
    narrow = jnp.where(lane < small, pltpu.roll(x, HEAD_DIM - small, 1), pltpu.roll(x, small, 1))
    return jnp.where(lane < 2 * small, narrow, wide)


def contract_first(a, b):
    return lax.dot_general(a, b, (((0,), (0,)), ((), ())), preferred_element_type=F32)


def contract_last(a, b):
    return lax.dot_general(a, b, (((1,), (1,)), ((), ())), preferred_element_type=F32)


def kernel(
    sizes,
    latent,
    positions,
    text_kv,
    text_len,
    modulation,
    w_qkv,
    gains,
    w_out,
    guidance,
    table,
    out,
    X,
    W,
    WO,
    T,
    A,
    Q,
    CT,
    ST,
    cs,
    bw,
    acc,
    lsum,
    KV,
    att,
    PO,
    G,
    RB,
    local_sem,
    zs,
    zr,
    xs,
    xr,
    dzs,
    dzr,
    dxs,
    dxr,
    ts,
    tr,
    As,
    Ar,
    wsend,
    wrecv,
    asend,
    arecv,
    gs,
    gr,
):
    n_seq, n_ten = sizes
    c = lax.axis_index("cfg")
    z = lax.axis_index("seq")
    x = lax.axis_index("tensor")
    par = lax.rem(x, 2)
    rows, d = latent.shape
    width = w_qkv.shape[2]
    heads = width // HEAD_DIM
    kdev = w_qkv.shape[1]
    half = rows // 2
    ch = half // 4
    own = n_seq - 1
    opp = n_seq - 2
    last_step = n_seq // 2
    n_ev = 4 * (last_step - 1) + 2
    first_last = 4 * (last_step - 1)
    z_up = lax.rem(z + 1, n_seq)
    z_down = lax.rem(z + n_seq - 1, n_seq)
    z_next = lax.rem(z + 1 - 2 * c + n_seq, n_seq)
    scale = HEAD_DIM**-0.5 * 1.4426950408889634

    def local(src, dst, k):
        return pltpu.make_async_copy(src, dst, local_sem.at[k])

    def remote(src, dst, ssem, rsem, device):
        return pltpu.make_async_remote_copy(
            src_ref=src,
            dst_ref=dst,
            send_sem=ssem,
            recv_sem=rsem,
            device_id=device,
            device_id_type=MESH,
        )

    mine_k = pl.ds(pl.multiple_of(c * kdev, kdev), kdev)
    other_k = pl.ds(pl.multiple_of((1 - c) * kdev, kdev), kdev)
    for j in range(3):
        local(w_qkv.at[j], W.at[j, mine_k], j).start()
    local(latent, X.at[own], 3).start()
    local(text_kv.at[0], T.at[own], 4).start()
    local(w_out, WO, 5).start()

    barrier = pltpu.get_barrier_semaphore()
    peers = [
        {"cfg": 1 - c},
        {"seq": z_up},
        {"seq": z_down},
        *({"tensor": lax.rem(x + k, n_ten)} for k in range(1, n_ten)),
    ]
    for peer in peers:
        pl.semaphore_signal(barrier, inc=1, device_id=peer, device_id_type=MESH)
    pl.semaphore_wait(barrier, len(peers))

    def chunk(e, core):
        is_last = e >= first_last
        idx = jnp.where(is_last, opp, 2 * lax.div(e, 4) + core)
        j = jnp.where(is_last, 2 * core + e - first_last, lax.rem(e, 4))
        return idx, j

    def row_of(j, parity):
        return pl.multiple_of(parity * half + j * ch, ch)

    def z_copy(src, idx, j, e):
        return remote(
            src,
            X.at[idx, pl.ds(row_of(j, par), ch)],
            zs.at[e],
            zr.at[e],
            {"seq": z_next},
        )

    def x_copy(e, parity):
        idx, j = chunk(e, c)
        back = jnp.where(e >= first_last, e - first_last, lax.div(j, 2))
        ref = X.at[idx, pl.ds(row_of(j, parity), ch)]
        to = lax.rem(x + 1 - 2 * back + n_ten, n_ten)
        return remote(ref, ref, xs.at[e], xr.at[e], {"tensor": to})

    def d_copy(e, core, parity, ssem, rsem):
        idx, j = chunk(e, core)
        ref = X.at[idx, pl.ds(row_of(j, parity), ch)]
        return remote(ref, ref, ssem.at[e], rsem.at[e], {"cfg": 1 - c})

    def z_event(e):
        idx, j = chunk(e, c)
        here = X.at[idx, pl.ds(row_of(j, par), ch)]
        z_copy(here, idx, j, e).wait_recv()
        going = (e < first_last - 4) | ((e < first_last) & (lax.div(j, 2) == c))

        @pl.when(going)
        def _():
            far = e >= first_last - 4
            ne = jnp.where(far, first_last + j - 2 * c, e + 4)
            nidx = jnp.where(far, opp, idx + 2)
            z_copy(here, nidx, j, ne).start()

        x_copy(e, par).start()
        d_copy(e, c, par, dzs, dzr).start()

    def x_event(e):
        x_copy(e, 1 - par).wait_recv()
        d_copy(e, c, 1 - par, dxs, dxr).start()

    def event(e):
        @pl.when(e < n_ev)
        def _():
            z_event(e)

        @pl.when((e >= 2) & (e < n_ev + 2))
        def _():
            x_event(e - 2)

    def t_copies(src, idx, direction):
        to = {"seq": z_down if direction else z_up}
        return (
            remote(T.at[src], T.at[idx], ts.at[idx], tr.at[idx], to),
            remote(A.at[src], A.at[idx], As.at[idx], Ar.at[idx], to),
        )

    def text_event(u):
        for direction in range(2):

            @pl.when((u < last_step) | (direction == 0))
            def _():
                idx = jnp.where(u < last_step, 2 * (u - 1) + direction, opp)
                for copy in t_copies(idx, idx, direction):
                    copy.wait_recv()

                @pl.when((u < last_step - 1) | ((u == last_step - 1) & (direction == 0)))
                def _():
                    nxt = jnp.where(u < last_step - 1, idx + 2, opp)
                    for copy in t_copies(idx, nxt, direction):
                        copy.start()

    for j in range(4):
        z_copy(latent.at[pl.ds(row_of(j, par), ch)], c, j, j).start()
    w_copies = [
        remote(w_qkv.at[j], W.at[j, mine_k], wsend.at[j], wrecv.at[j], {"cfg": 1 - c})
        for j in range(3)
    ]
    w_copies[2].start()
    local(text_kv.at[0], T.at[own], 4).wait()
    t_copies(own, 0, 0)[0].start()
    t_copies(own, 1, 1)[0].start()
    w_copies[1].start()
    w_copies[0].start()

    local(latent, X.at[own], 3).wait()
    xf = X[own].astype(F32)
    mean = jnp.mean(xf, axis=-1, keepdims=True)
    center = xf - mean
    rstd = lax.rsqrt(jnp.mean(center * center, axis=-1, keepdims=True) + 1e-06)
    lane = lax.broadcasted_iota(jnp.int32, (rows, HEAD_DIM), 1)
    stats = jnp.where(lane == 3, mean, jnp.where(lane == 4, rstd, 0.0))
    stats = jnp.transpose(stats)[0:8]
    sub = lax.broadcasted_iota(jnp.int32, (8, rows), 0)
    pos = positions[...].astype(F32)
    for k in range(3):
        stats = jnp.where(sub == k, pos[k : k + 1], stats)
    A[own] = stats
    t_copies(own, 0, 0)[1].start()
    t_copies(own, 1, 1)[1].start()

    kt = 256

    def fold(j, part):
        def body(i, carry):
            base = pl.multiple_of(part * kdev + i * kt, kt)
            shift_row = modulation[0, pl.ds(c, 1), pl.ds(base, kt)]
            scale_row = modulation[1, pl.ds(c, 1), pl.ds(base, kt)]
            srow = lax.broadcasted_iota(jnp.int32, (8, kt), 0)
            both = jnp.where(srow == 0, 1.0 + scale_row, jnp.where(srow == 1, shift_row, 0.0))
            cols = jnp.transpose(both)
            raw = W[j, pl.ds(base, kt), :].astype(F32)
            new = (raw * cols[:, 0:1]).astype(BF16)
            W[j, pl.ds(base, kt), :] = new
            cs[j] += jnp.sum(new.astype(F32).reshape(kt // 8, 8, width), axis=0)
            bw[j] += jnp.sum((raw * cols[:, 1:2]).reshape(kt // 8, 8, width), axis=0)
            return carry

        lax.fori_loop(0, kdev // kt, body, 0)

    def finish(j):
        cs[j] = jnp.broadcast_to(jnp.sum(cs[j], axis=0, keepdims=True), (8, width))
        bw[j] = jnp.broadcast_to(jnp.sum(bw[j], axis=0, keepdims=True), (8, width))

    cs[...] = jnp.zeros_like(cs)
    bw[...] = jnp.zeros_like(bw)
    acc[...] = jnp.zeros_like(acc)
    lsum[...] = jnp.zeros_like(lsum)
    for j in (2, 1, 0):
        local(w_qkv.at[j], W.at[j, mine_k], j).wait()
        fold(j, c)

    def w_arrive(j):
        remote(w_qkv.at[j], W.at[j, other_k], wsend.at[j], wrecv.at[j], {"cfg": 1 - c}).wait_recv()
        fold(j, 1 - c)
        finish(j)

    def tables(idx, at):
        a = A[idx]
        cols = jnp.transpose(a)
        at_rows = pl.ds(at, rows)
        rs = cols[:, 4:5]
        ST[0, at_rows] = jnp.broadcast_to(rs, (rows, HEAD_DIM))
        ST[1, at_rows] = jnp.broadcast_to(cols[:, 3:4] * rs, (rows, HEAD_DIM))
        index = lax.broadcasted_iota(jnp.int32, (TABLE_ROWS, rows), 0).astype(F32)
        hot = (
            (index == a[0:1] + float(STARTS[0]))
            | (index == a[1:2] + float(STARTS[1]))
            | (index == a[2:3] + float(STARTS[2]))
        )
        hot = jnp.where(hot, 1.0, 0.0).astype(BF16)
        CT[at_rows] = contract_first(hot, table[0:TABLE_ROWS]) + contract_first(
            hot, table[TABLE_ROWS : 2 * TABLE_ROWS]
        )

    def affine(block, j, lanes, m):
        return block * ST[0, 0:m] - ST[1, 0:m] * cs[j, 0:1, lanes] + bw[j, 0:1, lanes]

    def head_rows(block, j, lanes, m, gain):
        v = affine(block, j, lanes, m)
        r = lax.rsqrt(jnp.mean(v * v, axis=-1, keepdims=True) + 1e-06)
        v = v * gain
        v = v * CT[0:m, 0:HEAD_DIM] + partner_lanes(v) * CT[0:m, HEAD_DIM : 2 * HEAD_DIM]
        return (v * r).astype(BF16)

    q_gain = gains[0:1, :]
    k_gain = gains[1:2, :]

    def attend(h, keys, values, m, mask=None):
        s = contract_last(Q[h], keys)
        p = jnp.exp2(s * scale)
        if mask is not None:
            p = jnp.where(mask, p, 0.0)
        part = p[:, 0:HEAD_DIM]
        for k in range(1, m // HEAD_DIM):
            part = part + p[:, k * HEAD_DIM : (k + 1) * HEAD_DIM]
        lsum[h] += part
        acc[h] += jnp.dot(p.astype(BF16), values, preferred_element_type=F32)

    pair = 2 * HEAD_DIM

    def key_values(load, t, m):
        wide = slice(t * pair, (t + 1) * pair)
        k2 = jnp.dot(load(), W[1, :, wide], preferred_element_type=F32)
        v2 = jnp.dot(load(), W[2, :, wide], preferred_element_type=F32)
        for hh in range(2):
            h = 2 * t + hh
            lanes = slice(h * HEAD_DIM, (h + 1) * HEAD_DIM)
            sub_l = slice(hh * HEAD_DIM, (hh + 1) * HEAD_DIM)
            keys = head_rows(k2[:, sub_l], 1, lanes, m, k_gain)
            values = affine(v2[:, sub_l], 2, lanes, m).astype(BF16)
            attend(h, keys, values, m)

    event(0)
    w_arrive(2)
    tables(own, 0)
    event(1)
    text_event(1)
    w_arrive(1)
    event(2)
    w_arrive(0)
    event(3)
    for t in range(heads // 2):
        wide = slice(t * pair, (t + 1) * pair)
        q2 = jnp.dot(X[own], W[0, :, wide], preferred_element_type=F32)
        for hh in range(2):
            h = 2 * t + hh
            lanes = slice(h * HEAD_DIM, (h + 1) * HEAD_DIM)
            Q[h] = head_rows(
                q2[:, hh * HEAD_DIM : (hh + 1) * HEAD_DIM], 0, lanes, rows, q_gain
            )
    event(4)
    for t in range(heads // 2):
        key_values(lambda: X[own], t, rows)
    event(5)

    def wait_partner(e):
        d_copy(e, 1 - c, par, dzs, dzr).wait_recv()
        d_copy(e, 1 - c, 1 - par, dxs, dxr).wait_recv()

    def step(s, carry):
        def waits(k, carry):
            wait_partner(4 * (s - 1) + k)
            return carry

        lax.fori_loop(0, 4, waits, 0)
        base = pl.multiple_of(2 * (s - 1), 2)
        tables(base, 0)
        tables(base + 1, rows)
        for t in range(heads // 2):
            key_values(lambda: X[pl.ds(base, 2)].reshape(2 * rows, d), t, 2 * rows)
            event(4 * s + 2 + t)
        text_event(s + 1)
        event(4 * s + 5)
        return carry

    lax.fori_loop(1, last_step, step, 0)

    key_lane = lax.broadcasted_iota(jnp.int32, (1, n_seq * T.shape[2]), 1)
    trows = T.shape[2]
    slot = lax.div(key_lane, trows)
    away = lax.div(slot, 2) + 1
    sign = 1 - 2 * lax.rem(slot, 2)
    plane = lax.rem(z - sign * away + 2 * n_seq, n_seq)
    plane = jnp.where(slot == own, z, plane)
    plane = jnp.where(slot == opp, lax.rem(z + last_step, n_seq), plane)
    used = plane * trows + lax.rem(key_lane, trows) < text_len[0]
    m_text = n_seq * trows
    for h in range(heads):
        lanes = slice(h * HEAD_DIM, (h + 1) * HEAD_DIM)
        tk = T[:, 0, :, lanes].reshape(m_text, HEAD_DIM).astype(F32)
        r = lax.rsqrt(jnp.mean(tk * tk, axis=-1, keepdims=True) + 1e-06)
        keys = (tk * r * k_gain).astype(BF16)
        attend(h, keys, T[:, 1, :, lanes].reshape(m_text, HEAD_DIM), m_text, used)

    wait_partner(first_last)
    wait_partner(first_last + 1)
    tables(opp, 0)
    for t in range(heads // 2):
        key_values(lambda: X[opp], t, rows)

    for h in range(heads):
        total = jnp.sum(lsum[h], axis=-1, keepdims=True)
        att[0, :, h * HEAD_DIM : (h + 1) * HEAD_DIM] = (acc[h] / total).astype(BF16)
    swap = remote(att.at[0], att.at[1], asend.at[0], arecv.at[0], {"cfg": 1 - c})
    swap.start()
    local(w_out, WO, 5).wait()
    ocols = w_out.shape[1]
    mine_o = pl.multiple_of(c * ocols, ocols)
    nt = ocols // 3
    strength = guidance[0]
    cf = c.astype(F32)
    weight_own = strength * (1.0 - cf) + (1.0 - strength) * cf
    weight_other = 1.0 - weight_own
    for k in range(3):
        cols = slice(k * nt, (k + 1) * nt)
        PO[:, cols] = jnp.dot(att[0], WO[:, cols], preferred_element_type=F32)
    swap.wait()

    def g_copy(k, t):
        to = lax.rem(x + k, n_ten)
        qrows = rows // n_ten
        return remote(
            G.at[pl.ds(pl.multiple_of(to * qrows, qrows), qrows), pl.ds(t * nt, nt)],
            RB.at[k - 1, :, pl.ds(t * nt, nt)],
            gs.at[(k - 1) * 3 + t],
            gr.at[(k - 1) * 3 + t],
            {"tensor": to},
        )

    for t in range(3):
        cols = slice(t * nt, (t + 1) * nt)
        gate_own = modulation[2, pl.ds(c, 1), pl.ds(mine_o + t * nt, nt)]
        gate_other = modulation[2, pl.ds(1 - c, 1), pl.ds(mine_o + t * nt, nt)]
        other = jnp.dot(att[1], WO[:, cols], preferred_element_type=F32)
        G[:, cols] = (
            PO[:, cols] * (gate_own * weight_own) + other * (gate_other * weight_other)
        ).astype(BF16)
        for k in (2, 1, 3):
            g_copy(k, t).start()

    qrows = rows // n_ten
    for t in range(3):
        cols = slice(t * nt, (t + 1) * nt)
        total = G[pl.ds(pl.multiple_of(x * qrows, qrows), qrows), cols].astype(F32)
        for k in (1, 3, 2):
            g_copy(k, t).wait_recv()
            total = total + RB[k - 1, :, cols].astype(F32)
        out[:, cols] = total.astype(BF16)

    for t in range(3):
        for k in (1, 2, 3):
            g_copy(k, t).wait_send()
    for j in range(3):
        w_copies[j].wait_send()

    def sent(e, carry):
        x_copy(e, par).wait_send()
        d_copy(e, c, par, dzs, dzr).wait_send()
        d_copy(e, c, 1 - par, dxs, dxr).wait_send()
        idx, j = chunk(e, c)
        z_copy(X.at[idx, pl.ds(row_of(j, par), ch)], idx, j, e).wait_send()
        return carry

    lax.fori_loop(0, n_ev, sent, 0)

    def sent_text(idx, carry):
        for copy in t_copies(idx, idx, 0):
            copy.wait_send()
        return carry

    lax.fori_loop(0, own, sent_text, 0)


def solution(mesh):
    n_seq, n_ten = mesh.shape["seq"], mesh.shape["tensor"]

    def local(latent, positions, text_kv, text_len, modulation, w_qkv, gains, w_out, guidance):
        rows, d = latent.shape
        width = w_qkv.shape[2]
        heads = width // HEAD_DIM
        ocols = w_out.shape[1]
        n_ev = 4 * (n_seq // 2 - 1) + 2
        vmem, smem, anyw = pltpu.VMEM, pltpu.SMEM, pl.ANY
        spec = lambda space: pl.BlockSpec(memory_space=space)
        dma = pltpu.SemaphoreType.DMA
        return pl.pallas_call(
            functools.partial(kernel, (n_seq, n_ten)),
            out_shape=jax.ShapeDtypeStruct((rows // n_ten, ocols), BF16),
            in_specs=[
                spec(anyw),
                spec(vmem),
                spec(anyw),
                spec(smem),
                spec(vmem),
                spec(anyw),
                spec(vmem),
                spec(anyw),
                spec(smem),
                spec(vmem),
            ],
            out_specs=spec(vmem),
            scratch_shapes=[
                vmem((n_seq, rows, d), BF16),
                vmem((3, d, width), BF16),
                vmem((width, ocols), BF16),
                vmem((n_seq, 2, text_kv.shape[2], width), BF16),
                vmem((n_seq, 8, rows), F32),
                vmem((heads, rows, HEAD_DIM), BF16),
                vmem((2 * rows, 2 * HEAD_DIM), F32),
                vmem((2, 2 * rows, HEAD_DIM), F32),
                vmem((3, 8, width), F32),
                vmem((3, 8, width), F32),
                vmem((heads, rows, HEAD_DIM), F32),
                vmem((heads, rows, HEAD_DIM), F32),
                vmem((8, 128), F32),
                vmem((2, rows, width), BF16),
                vmem((rows, ocols), F32),
                vmem((rows, ocols), BF16),
                vmem((n_ten - 1, rows // n_ten, ocols), BF16),
                dma((6,)),
                dma((n_ev,)),
                dma((n_ev,)),
                dma((n_ev,)),
                dma((n_ev,)),
                dma((n_ev,)),
                dma((n_ev,)),
                dma((n_ev,)),
                dma((n_ev,)),
                dma((n_seq,)),
                dma((n_seq,)),
                dma((n_seq,)),
                dma((n_seq,)),
                dma((3,)),
                dma((3,)),
                dma((1,)),
                dma((1,)),
                dma((9,)),
                dma((9,)),
            ],
            compiler_params=pltpu.CompilerParams(
                collective_id=0, has_side_effects=True, vmem_limit_bytes=62 * 1024 * 1024
            ),
        )(
            latent,
            positions,
            text_kv,
            text_len,
            modulation,
            w_qkv,
            gains,
            w_out,
            guidance,
            rotary_table(),
        )

    placed = (
        P(("groups", "seq"), None),
        P(None, ("groups", "seq")),
        P("cfg", None, ("groups", "seq"), "tensor"),
        P(("groups", "cfg")),
        P(None, "groups", None),
        P(None, "cfg", "tensor"),
        P(),
        P("tensor", "cfg"),
        P("groups"),
    )
    return jax.shard_map(
        local,
        mesh=mesh,
        in_specs=placed,
        out_specs=P(("groups", "seq", "tensor"), "cfg"),
        check_vma=False,
    )
```

```python
import functools

import jax
import jax.numpy as jnp
import numpy as np
from jax import lax
from jax.experimental import pallas as pl
from jax.experimental.pallas import tpu as pltpu
from jax.sharding import PartitionSpec as P

HEAD_DIM = 128
MESH = pl.DeviceIdType.MESH
F32 = jnp.float32
BF16 = jnp.bfloat16
STARTS = (0, 40, 96)
LIMITS = (33, 45, 80)
TABLE_ROWS = 256
BLOCKS = (16, 56, 56)


def rotary_table():
    table = np.zeros((TABLE_ROWS, 2 * HEAD_DIM), np.float32)
    offset = 0
    for start, limit, width in zip(STARTS, LIMITS, BLOCKS):
        half = width // 2
        freq = (256.0 ** (-np.arange(half, dtype=np.float64) / half)).astype(np.float32)
        angle = np.arange(limit, dtype=np.float32)[:, None] * freq[None, :]
        cosine, sine = np.cos(angle.astype(np.float64)), np.sin(angle.astype(np.float64))
        rows = slice(start, start + limit)
        table[rows, offset : offset + half] = cosine
        table[rows, offset + half : offset + width] = cosine
        table[rows, HEAD_DIM + offset : HEAD_DIM + offset + half] = -sine
        table[rows, HEAD_DIM + offset + half : HEAD_DIM + offset + width] = sine
        offset += width
    high = jnp.asarray(table).astype(BF16)
    low = (jnp.asarray(table) - high.astype(F32)).astype(BF16)
    return jnp.concatenate([high, low], axis=0)


def partner_lanes(x):
    lane = lax.broadcasted_iota(jnp.int32, x.shape, 1)
    small, large = BLOCKS[0] // 2, BLOCKS[1] // 2
    wide_first = ((lane >= 16) & (lane < 44)) | ((lane >= 72) & (lane < 100))
    wide = jnp.where(
        wide_first, pltpu.roll(x, HEAD_DIM - large, 1), pltpu.roll(x, large, 1)
    )
    narrow = jnp.where(lane < small, pltpu.roll(x, HEAD_DIM - small, 1), pltpu.roll(x, small, 1))
    return jnp.where(lane < 2 * small, narrow, wide)


def contract_first(a, b):
    return lax.dot_general(a, b, (((0,), (0,)), ((), ())), preferred_element_type=F32)


def contract_last(a, b):
    return lax.dot_general(a, b, (((1,), (1,)), ((), ())), preferred_element_type=F32)


def kernel(
    sizes,
    latent,
    positions,
    text_kv,
    text_len,
    modulation,
    w_qkv,
    gains,
    w_out,
    guidance,
    table,
    out,
    X,
    XO,
    W,
    WO,
    T,
    A,
    Q,
    CT,
    ST,
    cs,
    bw,
    acc,
    lsum,
    KV,
    OW,
    att,
    PO,
    G,
    RB,
    local_sem,
    zs,
    zr,
    xs,
    xr,
    dzs,
    dzr,
    dxs,
    dxr,
    ts,
    tr,
    As,
    Ar,
    wsend,
    wrecv,
    asend,
    arecv,
    gs,
    gr,
):
    n_seq, n_ten = sizes
    c = lax.axis_index("cfg")
    z = lax.axis_index("seq")
    x = lax.axis_index("tensor")
    par = lax.rem(x, 2)
    rows, d = latent.shape
    width = w_qkv.shape[2]
    heads = width // HEAD_DIM
    kdev = w_qkv.shape[1]
    half = rows // 2
    ch = half // 4
    own = n_seq - 1
    opp = n_seq - 2
    last_step = n_seq // 2
    n_ev = 4 * (last_step - 1) + 2
    first_last = 4 * (last_step - 1)
    z_up = lax.rem(z + 1, n_seq)
    z_down = lax.rem(z + n_seq - 1, n_seq)
    scale = HEAD_DIM**-0.5 * 1.4426950408889634

    def local(src, dst, k):
        return pltpu.make_async_copy(src, dst, local_sem.at[k])

    def remote(src, dst, ssem, rsem, device):
        return pltpu.make_async_remote_copy(
            src_ref=src,
            dst_ref=dst,
            send_sem=ssem,
            recv_sem=rsem,
            device_id=device,
            device_id_type=MESH,
        )

    mine_k = pl.ds(pl.multiple_of(c * kdev, kdev), kdev)
    other_k = pl.ds(pl.multiple_of((1 - c) * kdev, kdev), kdev)
    pair = 2 * HEAD_DIM
    pairs = width // pair

    def w_from(t, j):
        return w_qkv.at[j, :, pl.ds(t * pair, pair)]

    def w_local(t, j):
        return local(w_from(t, j), W.at[t, mine_k, pl.ds(j * pair, pair)], 3 + 3 * t + j)

    local(latent, XO.at[pl.ds(0, rows)], 0).start()
    local(text_kv.at[0], T.at[own], 1).start()
    for t in range(pairs):
        for j in range(3):
            w_local(t, j).start()
    local(w_out, WO, 2).start()

    barrier = pltpu.get_barrier_semaphore()
    peers = [
        {"cfg": 1 - c},
        {"seq": z_up},
        {"seq": z_down},
        *({"tensor": lax.rem(x + k, n_ten)} for k in range(1, n_ten)),
    ]
    for peer in peers:
        pl.semaphore_signal(barrier, inc=1, device_id=peer, device_id_type=MESH)
    pl.semaphore_wait(barrier, len(peers))

    def chunk(e, core):
        is_last = e >= first_last
        k = lax.rem(e, 4)
        direction = lax.rem(k, 2)
        part = jnp.where(is_last, direction, lax.div(k, 2))
        idx = jnp.where(is_last, opp, 2 * lax.div(e, 4) + direction)
        return idx, 2 * core + part, direction, part

    def row_of(j, parity):
        return pl.multiple_of(parity * half + j * ch, ch)

    def z_copy(src, idx, j, direction, e):
        return remote(
            src,
            X.at[idx, pl.ds(row_of(j, par), ch)],
            zs.at[e],
            zr.at[e],
            {"seq": lax.rem(z + 1 - 2 * direction + n_seq, n_seq)},
        )

    def x_copy(e, parity):
        idx, j, _, part = chunk(e, c)
        ref = X.at[idx, pl.ds(row_of(j, parity), ch)]
        to = lax.rem(x + 1 - 2 * part + n_ten, n_ten)
        return remote(ref, ref, xs.at[e], xr.at[e], {"tensor": to})

    def d_copy(e, core, parity, ssem, rsem):
        idx, j, _, _ = chunk(e, core)
        ref = X.at[idx, pl.ds(row_of(j, parity), ch)]
        return remote(ref, ref, ssem.at[e], rsem.at[e], {"cfg": 1 - c})

    def z_event(e):
        idx, j, direction, part = chunk(e, c)
        here = X.at[idx, pl.ds(row_of(j, par), ch)]
        z_copy(here, idx, j, direction, e).wait_recv()
        going = (e < first_last - 4) | ((e < first_last) & (part == direction))

        @pl.when(going)
        def _():
            far = e >= first_last - 4
            ne = jnp.where(far, first_last + direction, e + 4)
            nidx = jnp.where(far, opp, idx + 2)
            z_copy(here, nidx, j, direction, ne).start()

        x_copy(e, par).start()
        d_copy(e, c, par, dzs, dzr).start()

    def x_event(e):
        x_copy(e, 1 - par).wait_recv()
        d_copy(e, c, 1 - par, dxs, dxr).start()

    lag = 4

    def event(e):
        @pl.when(e < n_ev)
        def _():
            z_event(e)

        @pl.when((e >= lag) & (e < n_ev + lag))
        def _():
            x_event(e - lag)

    def t_copies(src, idx, direction):
        to = {"seq": z_down if direction else z_up}
        return (
            remote(T.at[src], T.at[idx], ts.at[idx], tr.at[idx], to),
            remote(A.at[src], A.at[idx], As.at[idx], Ar.at[idx], to),
        )

    def text_event(u):
        for direction in range(2):

            @pl.when((u < last_step) | (direction == 0))
            def _():
                idx = jnp.where(u < last_step, 2 * (u - 1) + direction, opp)
                for copy in t_copies(idx, idx, direction):
                    copy.wait_recv()

                @pl.when((u < last_step - 1) | ((u == last_step - 1) & (direction == 0)))
                def _():
                    nxt = jnp.where(u < last_step - 1, idx + 2, opp)
                    for copy in t_copies(idx, nxt, direction):
                        copy.start()

    for k in range(4):
        j = 2 * c + k // 2
        z_copy(latent.at[pl.ds(row_of(j, par), ch)], k % 2, j, k % 2, k).start()
    def w_remote(t, j, k_rows):
        at = 3 * t + j
        return remote(
            w_from(t, j),
            W.at[t, k_rows, pl.ds(j * pair, pair)],
            wsend.at[at],
            wrecv.at[at],
            {"cfg": 1 - c},
        )

    for j in range(3):
        w_remote(0, j, mine_k).start()
    local(text_kv.at[0], T.at[own], 1).wait()
    t_copies(own, 0, 0)[0].start()
    t_copies(own, 1, 1)[0].start()
    for t in range(1, pairs):
        for j in range(3):
            w_remote(t, j, mine_k).start()

    local(latent, XO.at[pl.ds(0, rows)], 0).wait()
    XO[rows : rows + 16] = jnp.ones((16, d), BF16)
    xf = XO[0:rows].astype(F32)
    mean = jnp.mean(xf, axis=-1, keepdims=True)
    center = xf - mean
    rstd = lax.rsqrt(jnp.mean(center * center, axis=-1, keepdims=True) + 1e-06)
    lane = lax.broadcasted_iota(jnp.int32, (rows, HEAD_DIM), 1)
    stats = jnp.where(lane == 3, mean, jnp.where(lane == 4, rstd, 0.0))
    stats = jnp.transpose(stats)[0:8]
    sub = lax.broadcasted_iota(jnp.int32, (8, rows), 0)
    pos = positions[...].astype(F32)
    for k in range(3):
        stats = jnp.where(sub == k, pos[k : k + 1], stats)
    A[own] = stats
    t_copies(own, 0, 0)[1].start()
    t_copies(own, 1, 1)[1].start()

    kt = 256

    def fold(t, part):
        def body(i, carry):
            base = pl.multiple_of(part * kdev + i * kt, kt)
            shift_row = modulation[0, pl.ds(c, 1), pl.ds(base, kt)]
            scale_row = modulation[1, pl.ds(c, 1), pl.ds(base, kt)]
            srow = lax.broadcasted_iota(jnp.int32, (8, kt), 0)
            both = jnp.where(srow == 0, 1.0 + scale_row, jnp.where(srow == 1, shift_row, 0.0))
            cols = jnp.transpose(both)
            raw = W[t, pl.ds(base, kt), :].astype(F32)
            W[t, pl.ds(base, kt), :] = (raw * cols[:, 0:1]).astype(BF16)
            bw[t] += jnp.sum((raw * cols[:, 1:2]).reshape(kt // 8, 8, 3 * pair), axis=0)
            return carry

        lax.fori_loop(0, kdev // kt, body, 0)

    bw[...] = jnp.zeros_like(bw)
    acc[...] = jnp.zeros_like(acc)
    lsum[...] = jnp.zeros_like(lsum)

    def w_arrive(t):
        for j in range(3):
            w_remote(t, j, other_k).wait_recv()
        fold(t, 1 - c)
        bw[t] = jnp.broadcast_to(jnp.sum(bw[t], axis=0, keepdims=True), (8, 3 * pair))

    def tables(idx, at):
        a = A[idx]
        cols = jnp.transpose(a)
        at_rows = pl.ds(at, rows)
        rs = cols[:, 4:5]
        ST[0, at_rows] = jnp.broadcast_to(rs, (rows, HEAD_DIM))
        ST[1, at_rows] = jnp.broadcast_to(cols[:, 3:4] * rs, (rows, HEAD_DIM))
        index = lax.broadcasted_iota(jnp.int32, (TABLE_ROWS, rows), 0).astype(F32)
        hot = (
            (index == a[0:1] + float(STARTS[0]))
            | (index == a[1:2] + float(STARTS[1]))
            | (index == a[2:3] + float(STARTS[2]))
        )
        hot = jnp.where(hot, 1.0, 0.0).astype(BF16)
        CT[at_rows] = contract_first(hot, table[0:TABLE_ROWS]) + contract_first(
            hot, table[TABLE_ROWS : 2 * TABLE_ROWS]
        )

    q_gain = gains[0:1, :]
    k_gain = gains[1:2, :]

    def affine(block, t, lanes, m):
        return block * ST[0, 0:m] - ST[1, 0:m] * cs[t, 0:1, lanes] + bw[t, 0:1, lanes]

    def head_rows(block, t, lanes, m, gain):
        v = affine(block, t, lanes, m)
        r = lax.rsqrt(jnp.mean(v * v, axis=-1, keepdims=True) + 1e-06)
        v = v * gain
        v = v * CT[0:m, 0:HEAD_DIM] + partner_lanes(v) * CT[0:m, HEAD_DIM : 2 * HEAD_DIM]
        return v * r

    def attend(h, keys, values, m, mask=None):
        p = jnp.exp2(jnp.dot(keys, Q[h], preferred_element_type=F32) * scale)
        if mask is not None:
            p = jnp.where(mask, p, 0.0)
        lsum[h] += jnp.sum(p.reshape(m // 8, 8, rows), axis=0)
        acc[h] += contract_first(values, p.astype(BF16))

    def lanes_of(j, hh):
        return slice(j * pair + hh * HEAD_DIM, j * pair + (hh + 1) * HEAD_DIM)

    def attend_pair(kv, t, m, skip):
        for hh in range(2):
            kl, vl = lanes_of(1, hh), lanes_of(2, hh)
            k_in = slice(kl.start - skip, kl.stop - skip)
            v_in = slice(vl.start - skip, vl.stop - skip)
            keys = head_rows(kv[0:m, k_in], t, kl, m, k_gain).astype(BF16)
            values = affine(kv[0:m, v_in], t, vl, m).astype(BF16)
            attend(2 * t + hh, keys, values, m)

    def key_values(load, t, m):
        kv = jnp.dot(load(), W[t, :, pair : 3 * pair], preferred_element_type=F32)
        attend_pair(kv, t, m, pair)

    def own_dot(t):
        OW[t % 2] = jnp.dot(XO[...], W[t], preferred_element_type=F32)

    def own_pair(t):
        qkv = OW.at[t % 2]
        cs[t] = qkv[rows : rows + 8]
        for hh in range(2):
            ql = lanes_of(0, hh)
            q = head_rows(qkv[0:rows, ql], t, ql, rows, q_gain)
            Q[2 * t + hh] = jnp.transpose(q).astype(BF16)
        attend_pair(qkv, t, rows, 0)

    tables(own, 0)
    for t in range(pairs):
        for j in range(3):
            w_local(t, j).wait()
        fold(t, c)
        if t == 0:
            event(0)
    event(1)
    text_event(1)
    for t in range(pairs):
        w_arrive(t)
        event(2 * t + 2)
        own_dot(t)
        if t > 0:
            own_pair(t - 1)
        event(2 * t + 3)
    own_pair(pairs - 1)

    def wait_partner(e):
        d_copy(e, 1 - c, par, dzs, dzr).wait_recv()
        d_copy(e, 1 - c, 1 - par, dxs, dxr).wait_recv()

    def pair_dot(base, t):
        both = X[pl.ds(base, 2)].reshape(2 * rows, d)
        KV[t % 2] = jnp.dot(both, W[t, :, pair : 3 * pair], preferred_element_type=F32)

    def step(s, carry):
        def waits(k, carry):
            wait_partner(4 * (s - 1) + k)
            return carry

        lax.fori_loop(0, 4, waits, 0)
        base = pl.multiple_of(2 * (s - 1), 2)
        event(4 * s + 4)
        tables(base, 0)
        tables(base + 1, rows)
        pair_dot(base, 0)
        event(4 * s + 5)
        for t in range(1, pairs):
            pair_dot(base, t)
            attend_pair(KV.at[(t - 1) % 2], t - 1, 2 * rows, pair)
            event(4 * s + 5 + t)
        attend_pair(KV.at[(pairs - 1) % 2], pairs - 1, 2 * rows, pair)
        text_event(s + 1)
        return carry

    lax.fori_loop(1, last_step, step, 0)

    trows = T.shape[2]
    m_text = n_seq * trows
    key_row = lax.broadcasted_iota(jnp.int32, (m_text, rows), 0)
    slot = lax.div(key_row, trows)
    away = lax.div(slot, 2) + 1
    sign = 1 - 2 * lax.rem(slot, 2)
    plane = lax.rem(z - sign * away + 2 * n_seq, n_seq)
    plane = jnp.where(slot == own, z, plane)
    plane = jnp.where(slot == opp, lax.rem(z + last_step, n_seq), plane)
    used = plane * trows + lax.rem(key_row, trows) < text_len[0]
    for h in range(heads):
        lanes = slice(h * HEAD_DIM, (h + 1) * HEAD_DIM)
        tk = T[:, 0, :, lanes].reshape(m_text, HEAD_DIM).astype(F32)
        r = lax.rsqrt(jnp.mean(tk * tk, axis=-1, keepdims=True) + 1e-06)
        keys = (tk * r * k_gain).astype(BF16)
        attend(h, keys, T[:, 1, :, lanes].reshape(m_text, HEAD_DIM), m_text, used)

    wait_partner(first_last)
    wait_partner(first_last + 1)
    tables(opp, 0)
    for t in range(pairs):
        key_values(lambda: X[opp], t, rows)

    for h in range(heads):
        total = jnp.sum(lsum[h], axis=0, keepdims=True)
        mixed = jnp.transpose(acc[h] / total)
        att[0, :, h * HEAD_DIM : (h + 1) * HEAD_DIM] = mixed.astype(BF16)
    swap = remote(att.at[0], att.at[1], asend.at[0], arecv.at[0], {"cfg": 1 - c})
    swap.start()
    local(w_out, WO, 2).wait()
    ocols = w_out.shape[1]
    mine_o = pl.multiple_of(c * ocols, ocols)
    nt = ocols // 3
    strength = guidance[0]
    cf = c.astype(F32)
    weight_own = strength * (1.0 - cf) + (1.0 - strength) * cf
    weight_other = 1.0 - weight_own
    for k in range(3):
        cols = slice(k * nt, (k + 1) * nt)
        PO[:, cols] = jnp.dot(att[0], WO[:, cols], preferred_element_type=F32)
    swap.wait()

    def g_copy(k, t):
        to = lax.rem(x + k, n_ten)
        qrows = rows // n_ten
        return remote(
            G.at[pl.ds(pl.multiple_of(to * qrows, qrows), qrows), pl.ds(t * nt, nt)],
            RB.at[k - 1, :, pl.ds(t * nt, nt)],
            gs.at[(k - 1) * 3 + t],
            gr.at[(k - 1) * 3 + t],
            {"tensor": to},
        )

    for t in range(3):
        cols = slice(t * nt, (t + 1) * nt)
        gate_own = modulation[2, pl.ds(c, 1), pl.ds(mine_o + t * nt, nt)]
        gate_other = modulation[2, pl.ds(1 - c, 1), pl.ds(mine_o + t * nt, nt)]
        other = jnp.dot(att[1], WO[:, cols], preferred_element_type=F32)
        G[:, cols] = (
            PO[:, cols] * (gate_own * weight_own) + other * (gate_other * weight_other)
        ).astype(BF16)
        for k in (2, 1, 3):
            g_copy(k, t).start()

    qrows = rows // n_ten
    for t in range(3):
        cols = slice(t * nt, (t + 1) * nt)
        total = G[pl.ds(pl.multiple_of(x * qrows, qrows), qrows), cols].astype(F32)
        for k in (1, 3, 2):
            g_copy(k, t).wait_recv()
            total = total + RB[k - 1, :, cols].astype(F32)
        out[:, cols] = total.astype(BF16)

    for t in range(3):
        for k in (1, 2, 3):
            g_copy(k, t).wait_send()
    for t in range(pairs):
        for j in range(3):
            w_remote(t, j, mine_k).wait_send()

    def sent(e, carry):
        x_copy(e, par).wait_send()
        d_copy(e, c, par, dzs, dzr).wait_send()
        d_copy(e, c, 1 - par, dxs, dxr).wait_send()
        idx, j, direction, _ = chunk(e, c)
        z_copy(X.at[idx, pl.ds(row_of(j, par), ch)], idx, j, direction, e).wait_send()
        return carry

    lax.fori_loop(0, n_ev, sent, 0)

    def sent_text(idx, carry):
        for copy in t_copies(idx, idx, 0):
            copy.wait_send()
        return carry

    lax.fori_loop(0, own, sent_text, 0)


def solution(mesh):
    n_seq, n_ten = mesh.shape["seq"], mesh.shape["tensor"]

    def local(latent, positions, text_kv, text_len, modulation, w_qkv, gains, w_out, guidance):
        rows, d = latent.shape
        width = w_qkv.shape[2]
        heads = width // HEAD_DIM
        ocols = w_out.shape[1]
        n_ev = 4 * (n_seq // 2 - 1) + 2
        vmem, smem, anyw = pltpu.VMEM, pltpu.SMEM, pl.ANY
        spec = lambda space: pl.BlockSpec(memory_space=space)
        dma = pltpu.SemaphoreType.DMA
        return pl.pallas_call(
            functools.partial(kernel, (n_seq, n_ten)),
            out_shape=jax.ShapeDtypeStruct((rows // n_ten, ocols), BF16),
            in_specs=[
                spec(anyw),
                spec(vmem),
                spec(anyw),
                spec(smem),
                spec(vmem),
                spec(anyw),
                spec(vmem),
                spec(anyw),
                spec(smem),
                spec(vmem),
            ],
            out_specs=spec(vmem),
            scratch_shapes=[
                vmem((n_seq - 1, rows, d), BF16),
                vmem((rows + 16, d), BF16),
                vmem((heads // 2, d, 6 * HEAD_DIM), BF16),
                vmem((width, ocols), BF16),
                vmem((n_seq, 2, text_kv.shape[2], width), BF16),
                vmem((n_seq, 8, rows), F32),
                vmem((heads, HEAD_DIM, rows), BF16),
                vmem((2 * rows, 2 * HEAD_DIM), F32),
                vmem((2, 2 * rows, HEAD_DIM), F32),
                vmem((heads // 2, 8, 6 * HEAD_DIM), F32),
                vmem((heads // 2, 8, 6 * HEAD_DIM), F32),
                vmem((heads, HEAD_DIM, rows), F32),
                vmem((heads, 8, rows), F32),
                vmem((2, 2 * rows, 4 * HEAD_DIM), F32),
                vmem((2, rows + 16, 6 * HEAD_DIM), F32),
                vmem((2, rows, width), BF16),
                vmem((rows, ocols), F32),
                vmem((rows, ocols), BF16),
                vmem((n_ten - 1, rows // n_ten, ocols), BF16),
                dma((12,)),
                dma((n_ev,)),
                dma((n_ev,)),
                dma((n_ev,)),
                dma((n_ev,)),
                dma((n_ev,)),
                dma((n_ev,)),
                dma((n_ev,)),
                dma((n_ev,)),
                dma((n_seq,)),
                dma((n_seq,)),
                dma((n_seq,)),
                dma((n_seq,)),
                dma((9,)),
                dma((9,)),
                dma((1,)),
                dma((1,)),
                dma((9,)),
                dma((9,)),
            ],
            compiler_params=pltpu.CompilerParams(
                collective_id=0, has_side_effects=True, vmem_limit_bytes=62 * 1024 * 1024
            ),
        )(
            latent,
            positions,
            text_kv,
            text_len,
            modulation,
            w_qkv,
            gains,
            w_out,
            guidance,
            rotary_table(),
        )

    placed = (
        P(("groups", "seq"), None),
        P(None, ("groups", "seq")),
        P("cfg", None, ("groups", "seq"), "tensor"),
        P(("groups", "cfg")),
        P(None, "groups", None),
        P(None, "cfg", "tensor"),
        P(),
        P("tensor", "cfg"),
        P("groups"),
    )
    return jax.shard_map(
        local,
        mesh=mesh,
        in_specs=placed,
        out_specs=P(("groups", "seq", "tensor"), "cfg"),
        check_vma=False,
    )
```

```python
import functools

import jax
import jax.numpy as jnp
import numpy as np
from jax import lax
from jax.experimental import pallas as pl
from jax.experimental.pallas import tpu as pltpu
from jax.sharding import PartitionSpec as P

HEAD_DIM = 128
MESH = pl.DeviceIdType.MESH
F32 = jnp.float32
BF16 = jnp.bfloat16
STARTS = (0, 40, 96)
LIMITS = (33, 45, 80)
TABLE_ROWS = 256
BLOCKS = (16, 56, 56)


def rotary_table():
    table = np.zeros((TABLE_ROWS, 2 * HEAD_DIM), np.float32)
    offset = 0
    for start, limit, width in zip(STARTS, LIMITS, BLOCKS):
        half = width // 2
        freq = (256.0 ** (-np.arange(half, dtype=np.float64) / half)).astype(np.float32)
        angle = np.arange(limit, dtype=np.float32)[:, None] * freq[None, :]
        cosine, sine = np.cos(angle.astype(np.float64)), np.sin(angle.astype(np.float64))
        rows = slice(start, start + limit)
        table[rows, offset : offset + half] = cosine
        table[rows, offset + half : offset + width] = cosine
        table[rows, HEAD_DIM + offset : HEAD_DIM + offset + half] = -sine
        table[rows, HEAD_DIM + offset + half : HEAD_DIM + offset + width] = sine
        offset += width
    high = jnp.asarray(table).astype(BF16)
    low = (jnp.asarray(table) - high.astype(F32)).astype(BF16)
    return jnp.concatenate([high, low], axis=0)


def partner_lanes(x):
    lane = lax.broadcasted_iota(jnp.int32, x.shape, 1)
    small, large = BLOCKS[0] // 2, BLOCKS[1] // 2
    wide_first = ((lane >= 16) & (lane < 44)) | ((lane >= 72) & (lane < 100))
    wide = jnp.where(
        wide_first, pltpu.roll(x, HEAD_DIM - large, 1), pltpu.roll(x, large, 1)
    )
    narrow = jnp.where(lane < small, pltpu.roll(x, HEAD_DIM - small, 1), pltpu.roll(x, small, 1))
    return jnp.where(lane < 2 * small, narrow, wide)


def contract_first(a, b):
    return lax.dot_general(a, b, (((0,), (0,)), ((), ())), preferred_element_type=F32)


def contract_last(a, b):
    return lax.dot_general(a, b, (((1,), (1,)), ((), ())), preferred_element_type=F32)


def kernel(
    sizes,
    latent,
    positions,
    text_kv,
    text_len,
    modulation,
    w_qkv,
    gains,
    w_out,
    guidance,
    table,
    out,
    X,
    XO,
    W,
    WO,
    T,
    A,
    Q,
    CT,
    ST,
    cs,
    bw,
    acc,
    lsum,
    KV,
    OW,
    att,
    PO,
    G,
    RB,
    local_sem,
    zs,
    zr,
    xs,
    xr,
    dzs,
    dzr,
    dxs,
    dxr,
    ts,
    tr,
    As,
    Ar,
    wsend,
    wrecv,
    asend,
    arecv,
    gs,
    gr,
):
    n_seq, n_ten = sizes
    c = lax.axis_index("cfg")
    z = lax.axis_index("seq")
    x = lax.axis_index("tensor")
    par = lax.rem(x, 2)
    rows, d = latent.shape
    width = w_qkv.shape[2]
    heads = width // HEAD_DIM
    kdev = w_qkv.shape[1]
    half = rows // 2
    ch = half // 4
    own = n_seq - 1
    opp = n_seq - 2
    last_step = n_seq // 2
    n_ev = 4 * (last_step - 1) + 2
    first_last = 4 * (last_step - 1)
    z_up = lax.rem(z + 1, n_seq)
    z_down = lax.rem(z + n_seq - 1, n_seq)
    scale = HEAD_DIM**-0.5 * 1.4426950408889634

    def local(src, dst, k):
        return pltpu.make_async_copy(src, dst, local_sem.at[k])

    def remote(src, dst, ssem, rsem, device):
        return pltpu.make_async_remote_copy(
            src_ref=src,
            dst_ref=dst,
            send_sem=ssem,
            recv_sem=rsem,
            device_id=device,
            device_id_type=MESH,
        )

    mine_k = pl.ds(pl.multiple_of(c * kdev, kdev), kdev)
    other_k = pl.ds(pl.multiple_of((1 - c) * kdev, kdev), kdev)
    pair = 2 * HEAD_DIM
    pairs = width // pair

    def w_from(t, j):
        return w_qkv.at[j, :, pl.ds(t * pair, pair)]

    def w_local(t, j):
        return local(w_from(t, j), W.at[t, mine_k, pl.ds(j * pair, pair)], 3 + 3 * t + j)

    local(latent, XO.at[pl.ds(0, rows)], 0).start()
    local(text_kv.at[0], T.at[own], 1).start()
    for t in range(pairs):
        for j in range(3):
            w_local(t, j).start()
    local(w_out, WO, 2).start()
    local(latent, X.at[own], 12).start()

    barrier = pltpu.get_barrier_semaphore()
    peers = [
        {"cfg": 1 - c},
        {"seq": z_up},
        {"seq": z_down},
        *({"tensor": lax.rem(x + k, n_ten)} for k in range(1, n_ten)),
    ]
    for peer in peers:
        pl.semaphore_signal(barrier, inc=1, device_id=peer, device_id_type=MESH)
    pl.semaphore_wait(barrier, len(peers))

    def chunk(e, core):
        is_last = e >= first_last
        k = lax.rem(e, 4)
        direction = lax.rem(k, 2)
        part = jnp.where(is_last, direction, lax.div(k, 2))
        idx = jnp.where(is_last, opp, 2 * lax.div(e, 4) + direction)
        return idx, 2 * core + part, direction, part

    def row_of(j, parity):
        return pl.multiple_of(parity * half + j * ch, ch)

    def z_copy(src, idx, j, direction, e):
        return remote(
            src,
            X.at[idx, pl.ds(row_of(j, par), ch)],
            zs.at[e],
            zr.at[e],
            {"seq": lax.rem(z + 1 - 2 * direction + n_seq, n_seq)},
        )

    def x_copy(e, parity):
        idx, j, _, part = chunk(e, c)
        ref = X.at[idx, pl.ds(row_of(j, parity), ch)]
        to = lax.rem(x + 1 - 2 * part + n_ten, n_ten)
        return remote(ref, ref, xs.at[e], xr.at[e], {"tensor": to})

    def d_copy(e, core, parity, ssem, rsem):
        idx, j, _, _ = chunk(e, core)
        ref = X.at[idx, pl.ds(row_of(j, parity), ch)]
        return remote(ref, ref, ssem.at[e], rsem.at[e], {"cfg": 1 - c})

    def z_event(e):
        idx, j, direction, part = chunk(e, c)
        here = X.at[idx, pl.ds(row_of(j, par), ch)]
        z_copy(here, idx, j, direction, e).wait_recv()
        going = (e < first_last - 4) | ((e < first_last) & (part == direction))

        @pl.when(going)
        def _():
            far = e >= first_last - 4
            ne = jnp.where(far, first_last + direction, e + 4)
            nidx = jnp.where(far, opp, idx + 2)
            z_copy(here, nidx, j, direction, ne).start()

        x_copy(e, par).start()
        d_copy(e, c, par, dzs, dzr).start()

    def x_event(e):
        x_copy(e, 1 - par).wait_recv()
        d_copy(e, c, 1 - par, dxs, dxr).start()

    lag = 4

    def event(e):
        @pl.when(e < n_ev)
        def _():
            z_event(e)

        @pl.when((e >= lag) & (e < n_ev + lag))
        def _():
            x_event(e - lag)

    def t_copies(src, idx, direction):
        to = {"seq": z_down if direction else z_up}
        return (
            remote(T.at[src], T.at[idx], ts.at[idx], tr.at[idx], to),
            remote(A.at[src], A.at[idx], As.at[idx], Ar.at[idx], to),
        )

    def text_event(u):
        for direction in range(2):

            @pl.when((u < last_step) | (direction == 0))
            def _():
                idx = jnp.where(u < last_step, 2 * (u - 1) + direction, opp)
                for copy in t_copies(idx, idx, direction):
                    copy.wait_recv()

                @pl.when((u < last_step - 1) | ((u == last_step - 1) & (direction == 0)))
                def _():
                    nxt = jnp.where(u < last_step - 1, idx + 2, opp)
                    for copy in t_copies(idx, nxt, direction):
                        copy.start()

    for k in range(4):
        j = 2 * c + k // 2
        z_copy(latent.at[pl.ds(row_of(j, par), ch)], k % 2, j, k % 2, k).start()
    def w_remote(t, j, k_rows):
        at = 3 * t + j
        return remote(
            w_from(t, j),
            W.at[t, k_rows, pl.ds(j * pair, pair)],
            wsend.at[at],
            wrecv.at[at],
            {"cfg": 1 - c},
        )

    for j in range(3):
        w_remote(0, j, mine_k).start()
    local(text_kv.at[0], T.at[own], 1).wait()
    t_copies(own, 0, 0)[0].start()
    t_copies(own, 1, 1)[0].start()
    for t in range(1, pairs):
        for j in range(3):
            w_remote(t, j, mine_k).start()

    local(latent, XO.at[pl.ds(0, rows)], 0).wait()
    XO[rows : rows + 16] = jnp.ones((16, d), BF16)
    xf = XO[0:rows].astype(F32)
    mean = jnp.mean(xf, axis=-1, keepdims=True)
    center = xf - mean
    rstd = lax.rsqrt(jnp.mean(center * center, axis=-1, keepdims=True) + 1e-06)
    lane = lax.broadcasted_iota(jnp.int32, (rows, HEAD_DIM), 1)
    stats = jnp.where(lane == 3, mean, jnp.where(lane == 4, rstd, 0.0))
    stats = jnp.transpose(stats)[0:8]
    sub = lax.broadcasted_iota(jnp.int32, (8, rows), 0)
    pos = positions[...].astype(F32)
    for k in range(3):
        stats = jnp.where(sub == k, pos[k : k + 1], stats)
    A[own] = stats
    t_copies(own, 0, 0)[1].start()
    t_copies(own, 1, 1)[1].start()

    kt = 256

    def fold(t, part):
        def body(i, carry):
            base = pl.multiple_of(part * kdev + i * kt, kt)
            shift_row = modulation[0, pl.ds(c, 1), pl.ds(base, kt)]
            scale_row = modulation[1, pl.ds(c, 1), pl.ds(base, kt)]
            srow = lax.broadcasted_iota(jnp.int32, (8, kt), 0)
            both = jnp.where(srow == 0, 1.0 + scale_row, jnp.where(srow == 1, shift_row, 0.0))
            cols = jnp.transpose(both)
            raw = W[t, pl.ds(base, kt), :].astype(F32)
            W[t, pl.ds(base, kt), :] = (raw * cols[:, 0:1]).astype(BF16)
            bw[t] += jnp.sum((raw * cols[:, 1:2]).reshape(kt // 8, 8, 3 * pair), axis=0)
            return carry

        lax.fori_loop(0, kdev // kt, body, 0)

    bw[...] = jnp.zeros_like(bw)
    acc[...] = jnp.zeros_like(acc)
    lsum[...] = jnp.zeros_like(lsum)

    def w_arrive(t):
        for j in range(3):
            w_remote(t, j, other_k).wait_recv()
        fold(t, 1 - c)
        bw[t] = jnp.broadcast_to(jnp.sum(bw[t], axis=0, keepdims=True), (8, 3 * pair))

    def tables(idx, at, q):
        a = A[idx]
        cols = jnp.transpose(a)
        at_rows = pl.ds(at, rows)
        rs = cols[:, 4:5]
        ST[q, 0, at_rows] = jnp.broadcast_to(rs, (rows, HEAD_DIM))
        ST[q, 1, at_rows] = jnp.broadcast_to(cols[:, 3:4] * rs, (rows, HEAD_DIM))
        index = lax.broadcasted_iota(jnp.int32, (TABLE_ROWS, rows), 0).astype(F32)
        hot = (
            (index == a[0:1] + float(STARTS[0]))
            | (index == a[1:2] + float(STARTS[1]))
            | (index == a[2:3] + float(STARTS[2]))
        )
        hot = jnp.where(hot, 1.0, 0.0).astype(BF16)
        CT[q, at_rows] = contract_first(hot, table[0:TABLE_ROWS]) + contract_first(
            hot, table[TABLE_ROWS : 2 * TABLE_ROWS]
        )

    q_gain = gains[0:1, :]
    k_gain = gains[1:2, :]

    def affine(block, t, lanes, m, q):
        return block * ST[q, 0, 0:m] - ST[q, 1, 0:m] * cs[t, 0:1, lanes] + bw[t, 0:1, lanes]

    def head_rows(block, t, lanes, m, gain, q):
        v = affine(block, t, lanes, m, q)
        r = lax.rsqrt(jnp.mean(v * v, axis=-1, keepdims=True) + 1e-06)
        v = v * gain
        v = v * CT[q, 0:m, 0:HEAD_DIM] + partner_lanes(v) * CT[q, 0:m, HEAD_DIM : 2 * HEAD_DIM]
        return v * r

    def attend(h, keys, values, m, mask=None):
        p = jnp.exp2(jnp.dot(keys, Q[h], preferred_element_type=F32) * scale)
        if mask is not None:
            p = jnp.where(mask, p, 0.0)
        lsum[h] += jnp.sum(p.reshape(m // 8, 8, rows), axis=0)
        acc[h] += contract_first(values, p.astype(BF16))

    def lanes_of(j, hh):
        return slice(j * pair + hh * HEAD_DIM, j * pair + (hh + 1) * HEAD_DIM)

    def attend_pair(kv, t, m, skip, q):
        for hh in range(2):
            kl, vl = lanes_of(1, hh), lanes_of(2, hh)
            k_in = slice(kl.start - skip, kl.stop - skip)
            v_in = slice(vl.start - skip, vl.stop - skip)
            keys = head_rows(kv[0:m, k_in], t, kl, m, k_gain, q).astype(BF16)
            values = affine(kv[0:m, v_in], t, vl, m, q).astype(BF16)
            attend(2 * t + hh, keys, values, m)

    def own_dot(t):
        OW[t % 2] = jnp.dot(XO[...], W[t], preferred_element_type=F32)

    def own_pair(t):
        qkv = OW.at[t % 2]
        cs[t] = qkv[rows : rows + 8]
        for hh in range(2):
            ql = lanes_of(0, hh)
            query = head_rows(qkv[0:rows, ql], t, ql, rows, q_gain, 0)
            Q[2 * t + hh] = jnp.transpose(query).astype(BF16)
        attend_pair(qkv, t, rows, 0, 0)

    tables(own, 0, 0)
    for t in range(pairs):
        for j in range(3):
            w_local(t, j).wait()
        fold(t, c)
        if t == 0:
            event(0)
    event(1)
    text_event(1)
    for t in range(pairs):
        w_arrive(t)
        event(2 * t + 2)
        own_dot(t)
        if t > 0:
            own_pair(t - 1)
        event(2 * t + 3)
    def wait_partner(e):
        d_copy(e, 1 - c, par, dzs, dzr).wait_recv()
        d_copy(e, 1 - c, 1 - par, dxs, dxr).wait_recv()

    def pair_dot(base, t):
        both = X[pl.ds(base, 2)].reshape(2 * rows, d)
        KV[t] = jnp.dot(both, W[t, :, pair : 3 * pair], preferred_element_type=F32)

    def begin(s):
        def waits(k, carry):
            e = 4 * (s - 1) + k

            @pl.when(e < n_ev)
            def _():
                wait_partner(e)

            return carry

        lax.fori_loop(0, 4, waits, 0)

    def first_dot(s, q):
        base = pl.multiple_of(2 * (s - 1), 2)
        tables(base, 0, q)
        tables(base + 1, rows, q)
        pair_dot(base, 0)

    last = pairs - 1
    local(latent, X.at[own], 12).wait()
    begin(1)
    first_dot(1, 1)
    own_pair(last)

    def prompt_rows():
        trows = T.shape[2]
        m_text = n_seq * trows
        key_row = lax.broadcasted_iota(jnp.int32, (m_text, rows), 0)
        slot = lax.div(key_row, trows)
        away = lax.div(slot, 2) + 1
        sign = 1 - 2 * lax.rem(slot, 2)
        plane = lax.rem(z - sign * away + 2 * n_seq, n_seq)
        plane = jnp.where(slot == own, z, plane)
        plane = jnp.where(slot == opp, lax.rem(z + last_step, n_seq), plane)
        used = plane * trows + lax.rem(key_row, trows) < text_len[0]
        for h in range(heads):
            lanes = slice(h * HEAD_DIM, (h + 1) * HEAD_DIM)
            tk = T[:, 0, :, lanes].reshape(m_text, HEAD_DIM).astype(F32)
            r = lax.rsqrt(jnp.mean(tk * tk, axis=-1, keepdims=True) + 1e-06)
            keys = (tk * r * k_gain).astype(BF16)
            attend(h, keys, T[:, 1, :, lanes].reshape(m_text, HEAD_DIM), m_text, used)

    def step(s, carry):
        base = pl.multiple_of(2 * (s - 1), 2)
        q = lax.rem(s, 2)
        for t in range(1, pairs):
            event(4 * s + 3 + t)
            pair_dot(base, t)
            attend_pair(KV.at[t - 1], t - 1, 2 * rows, pair, q)
        event(4 * s + 6)
        text_event(s + 1)
        event(4 * s + 7)

        @pl.when(s == last_step - 1)
        def _():
            prompt_rows()

        begin(s + 1)
        first_dot(s + 1, 1 - q)
        attend_pair(KV.at[last], last, 2 * rows, pair, q)
        return carry

    lax.fori_loop(1, last_step, step, 0)

    for t in range(pairs):
        if t > 0:
            KV[t, 0:rows] = jnp.dot(X[opp], W[t, :, pair : 3 * pair], preferred_element_type=F32)
        attend_pair(KV.at[t], t, rows, pair, last_step % 2)

    for h in range(heads):
        total = jnp.sum(lsum[h], axis=0, keepdims=True)
        mixed = jnp.transpose(acc[h] / total)
        att[0, :, h * HEAD_DIM : (h + 1) * HEAD_DIM] = mixed.astype(BF16)
    swap = remote(att.at[0], att.at[1], asend.at[0], arecv.at[0], {"cfg": 1 - c})
    swap.start()
    local(w_out, WO, 2).wait()
    ocols = w_out.shape[1]
    mine_o = pl.multiple_of(c * ocols, ocols)
    nt = ocols // 3
    strength = guidance[0]
    cf = c.astype(F32)
    weight_own = strength * (1.0 - cf) + (1.0 - strength) * cf
    weight_other = 1.0 - weight_own
    for k in range(3):
        cols = slice(k * nt, (k + 1) * nt)
        PO[:, cols] = jnp.dot(att[0], WO[:, cols], preferred_element_type=F32)
    swap.wait()

    def g_copy(k, t):
        to = lax.rem(x + k, n_ten)
        qrows = rows // n_ten
        return remote(
            G.at[pl.ds(pl.multiple_of(to * qrows, qrows), qrows), pl.ds(t * nt, nt)],
            RB.at[k - 1, :, pl.ds(t * nt, nt)],
            gs.at[(k - 1) * 3 + t],
            gr.at[(k - 1) * 3 + t],
            {"tensor": to},
        )

    for t in range(3):
        cols = slice(t * nt, (t + 1) * nt)
        gate_own = modulation[2, pl.ds(c, 1), pl.ds(mine_o + t * nt, nt)]
        gate_other = modulation[2, pl.ds(1 - c, 1), pl.ds(mine_o + t * nt, nt)]
        other = jnp.dot(att[1], WO[:, cols], preferred_element_type=F32)
        G[:, cols] = (
            PO[:, cols] * (gate_own * weight_own) + other * (gate_other * weight_other)
        ).astype(BF16)
        for k in (2, 1, 3):
            g_copy(k, t).start()

    qrows = rows // n_ten
    for t in range(3):
        cols = slice(t * nt, (t + 1) * nt)
        total = G[pl.ds(pl.multiple_of(x * qrows, qrows), qrows), cols].astype(F32)
        for k in (1, 3, 2):
            g_copy(k, t).wait_recv()
            total = total + RB[k - 1, :, cols].astype(F32)
        out[:, cols] = total.astype(BF16)

    for t in range(3):
        for k in (1, 2, 3):
            g_copy(k, t).wait_send()
    for t in range(pairs):
        for j in range(3):
            w_remote(t, j, mine_k).wait_send()

    def sent(e, carry):
        x_copy(e, par).wait_send()
        d_copy(e, c, par, dzs, dzr).wait_send()
        d_copy(e, c, 1 - par, dxs, dxr).wait_send()
        idx, j, direction, _ = chunk(e, c)
        z_copy(X.at[idx, pl.ds(row_of(j, par), ch)], idx, j, direction, e).wait_send()
        return carry

    lax.fori_loop(0, n_ev, sent, 0)

    def sent_text(idx, carry):
        for copy in t_copies(idx, idx, 0):
            copy.wait_send()
        return carry

    lax.fori_loop(0, own, sent_text, 0)


def solution(mesh):
    n_seq, n_ten = mesh.shape["seq"], mesh.shape["tensor"]

    def local(latent, positions, text_kv, text_len, modulation, w_qkv, gains, w_out, guidance):
        rows, d = latent.shape
        width = w_qkv.shape[2]
        heads = width // HEAD_DIM
        ocols = w_out.shape[1]
        n_ev = 4 * (n_seq // 2 - 1) + 2
        vmem, smem, anyw = pltpu.VMEM, pltpu.SMEM, pl.ANY
        spec = lambda space: pl.BlockSpec(memory_space=space)
        dma = pltpu.SemaphoreType.DMA
        return pl.pallas_call(
            functools.partial(kernel, (n_seq, n_ten)),
            out_shape=jax.ShapeDtypeStruct((rows // n_ten, ocols), BF16),
            in_specs=[
                spec(anyw),
                spec(vmem),
                spec(anyw),
                spec(smem),
                spec(vmem),
                spec(anyw),
                spec(vmem),
                spec(anyw),
                spec(smem),
                spec(vmem),
            ],
            out_specs=spec(vmem),
            scratch_shapes=[
                vmem((n_seq, rows, d), BF16),
                vmem((rows + 16, d), BF16),
                vmem((heads // 2, d, 6 * HEAD_DIM), BF16),
                vmem((width, ocols), BF16),
                vmem((n_seq, 2, text_kv.shape[2], width), BF16),
                vmem((n_seq, 8, rows), F32),
                vmem((heads, HEAD_DIM, rows), BF16),
                vmem((2, 2 * rows, 2 * HEAD_DIM), F32),
                vmem((2, 2, 2 * rows, HEAD_DIM), F32),
                vmem((heads // 2, 8, 6 * HEAD_DIM), F32),
                vmem((heads // 2, 8, 6 * HEAD_DIM), F32),
                vmem((heads, HEAD_DIM, rows), F32),
                vmem((heads, 8, rows), F32),
                vmem((heads // 2, 2 * rows, 4 * HEAD_DIM), F32),
                vmem((2, rows + 16, 6 * HEAD_DIM), F32),
                vmem((2, rows, width), BF16),
                vmem((rows, ocols), F32),
                vmem((rows, ocols), BF16),
                vmem((n_ten - 1, rows // n_ten, ocols), BF16),
                dma((13,)),
                dma((n_ev,)),
                dma((n_ev,)),
                dma((n_ev,)),
                dma((n_ev,)),
                dma((n_ev,)),
                dma((n_ev,)),
                dma((n_ev,)),
                dma((n_ev,)),
                dma((n_seq,)),
                dma((n_seq,)),
                dma((n_seq,)),
                dma((n_seq,)),
                dma((9,)),
                dma((9,)),
                dma((1,)),
                dma((1,)),
                dma((9,)),
                dma((9,)),
            ],
            compiler_params=pltpu.CompilerParams(
                collective_id=0, has_side_effects=True, vmem_limit_bytes=62 * 1024 * 1024
            ),
        )(
            latent,
            positions,
            text_kv,
            text_len,
            modulation,
            w_qkv,
            gains,
            w_out,
            guidance,
            rotary_table(),
        )

    placed = (
        P(("groups", "seq"), None),
        P(None, ("groups", "seq")),
        P("cfg", None, ("groups", "seq"), "tensor"),
        P(("groups", "cfg")),
        P(None, "groups", None),
        P(None, "cfg", "tensor"),
        P(),
        P("tensor", "cfg"),
        P("groups"),
    )
    return jax.shard_map(
        local,
        mesh=mesh,
        in_specs=placed,
        out_specs=P(("groups", "seq", "tensor"), "cfg"),
        check_vma=False,
    )
```
